32 devices in a mesh: ep: 4 (over y, x), fsdp: 8 (over z, core).
Axes of the slice: x: 2, y: 2, z: 4, core: 2. Of those that a mesh axis runs over, the one named last changes fastest.
Arguments:
- train_gate: float32 [64, 2048, 1408], P('ep', 'fsdp'), may hold values from -0.1875 to 0.1875
- other_gate: bfloat16 [64, 2048, 1408], P('ep', 'fsdp'), may hold values from -0.0625 to 0.0625
- train_up: float32 [64, 2048, 1408], P('ep', 'fsdp'), may hold values from -0.1875 to 0.1875
- other_up: bfloat16 [64, 2048, 1408], P('ep', 'fsdp'), may hold values from -0.0625 to 0.0625
- router_weight: float32 [2048, 64], P('fsdp', 'ep'), may hold values from -0.125 to 0.125
- router_gain: float32 [2048], P('fsdp'), may hold values from 0.25 to 1.75
Outputs:
- ready_gate: bfloat16 [64, 2048, 1408], P('ep', None, 'fsdp')
- ready_up: bfloat16 [64, 2048, 1408], P('ep', None, 'fsdp')
- scale_gate: float32 [64, 1408], P('ep', 'fsdp')
- scale_up: float32 [64, 1408], P('ep', 'fsdp')
- serve_router: bfloat16 [2048, 64], replicated
The draws below stay inside these ranges and needn't reach their ends.
All inputs are finite; a program needn't handle non-finite values. Where the reference program divides by a largest or mean magnitude, that divisor is 1e-20 or more.
Results may differ from the reference program's by a relative error of at most 0.001.
Values may be sent and summed in bfloat16 or wider, within the bound.
A program may use at most 192 MiB of HBM per device.

```python
import jax
import jax.numpy as jnp

EXPERTS = 64
D_MODEL = 2048
D_EXPERT = 1408


def strengthened(array, stream_key, source, target, blocks, factor):
    owner, partner = [(jnp.arange(array.shape[axis_at]) // (array.shape[axis_at] // blocks)).reshape([-1 if axis == axis_at else 1 for axis in range(array.ndim)]) for axis_at in (source, target)]
    chosen = jax.random.permutation(stream_key, blocks)[partner]
    strong = (owner == chosen) | (owner == (partner + blocks // 2) % blocks)
    return jnp.where(strong, factor * array, array)


def steps_of(rng, shape, split, smallest, high):
    def one(axis_at, shards_of):
        heights = jax.random.uniform(jax.random.fold_in(jax.random.fold_in(rng, 6), axis_at), (shards_of,), jnp.float32, smallest / len(split), high / len(split))
        return jnp.repeat(jnp.exp(heights), shape[axis_at] // shards_of).reshape((-1,) + (1,) * (len(shape) - axis_at - 1))

    factor_of = one(*split[0])
    for cut in split[1:]:
        factor_of = factor_of * one(*cut)
    return factor_of


def normal_values(own_key, extent, spread, limit, cuts=(), held_as=jnp.bfloat16):
    entries = spread * jax.random.normal(own_key, extent, jnp.float32)
    if cuts:
        entries = entries * steps_of(own_key, extent, cuts, -0.22, 0.18)
    return jnp.clip(entries, -limit, limit).astype(held_as)


def bell_draw_with(stream_key, shape, spread, most, split, heavy, dtype=jnp.bfloat16):
    result = spread * jax.random.normal(stream_key, shape, jnp.float32)
    if split:
        result = result * steps_of(stream_key, shape, split, -0.22, 0.18)
    return jnp.clip(strengthened(result, jax.random.fold_in(stream_key, 3), *heavy), -most, most).astype(dtype)


def setup_inputs(seed: int = 0) -> dict:
    splits = jax.random.split(jax.random.key(seed), 7)
    train_gate = bell_draw_with(splits[0], (EXPERTS, D_MODEL, D_EXPERT), D_MODEL ** -0.5, 0.1875, ((0, 4), (1, 8)), (1, 2, 8, 2.0), jnp.float32)
    other_gate = normal_values(splits[1], (EXPERTS, D_MODEL, D_EXPERT), (D_MODEL * 4) ** -0.5, 0.0625, ((0, 4), (1, 8)))
    train_up = bell_draw_with(splits[2], (EXPERTS, D_MODEL, D_EXPERT), D_MODEL ** -0.5, 0.1875, ((0, 4), (1, 8)), (1, 2, 8, 2.0), jnp.float32)
    other_up = normal_values(splits[3], (EXPERTS, D_MODEL, D_EXPERT), (D_MODEL * 4) ** -0.5, 0.0625, ((0, 4), (1, 8)))
    router_weight = normal_values(splits[4], (D_MODEL, EXPERTS), D_MODEL ** -0.5, 0.125, ((0, 8), (1, 4)), jnp.float32)
    router_gain = jnp.clip(1.0 + 0.15 * jax.random.normal(splits[5], (D_MODEL,), jnp.float32), 0.25, 1.75)
    return dict(train_gate=train_gate, other_gate=other_gate, train_up=train_up, other_up=other_up, router_weight=router_weight, router_gain=router_gain)


def reference(train_gate, other_gate, train_up, other_up, router_weight, router_gain):
    latest_gate = train_gate + other_gate.astype(jnp.float32)
    latest_up = train_up + other_up.astype(jnp.float32)
    scale_gate = jnp.max(jnp.abs(latest_gate), axis=1)
    ready_gate = (latest_gate / jnp.expand_dims(scale_gate, 1)).astype(jnp.bfloat16)
    scale_up = jnp.max(jnp.abs(latest_up), axis=1)
    ready_up = (latest_up / jnp.expand_dims(scale_up, 1)).astype(jnp.bfloat16)
    serve_router = (router_weight * router_gain[:, None]).astype(jnp.bfloat16)
    return ready_gate, ready_up, scale_gate, scale_up, serve_router
```

```python
import functools

import jax
import jax.numpy as jnp
from jax import lax
from jax.experimental import pallas as pl
from jax.experimental.pallas import tpu as pltpu
from jax.sharding import PartitionSpec as P

LANES = 128
DEPTH = 3


def regroup(n, tg, og, tu, ou, rg, ru, scales, mx, mo, nx, no, turned, blocks, own, pair, both, chips, final,
            mx_sem, mo_sem, nx_sem, no_sem, send_sem, keep_sem, recv_sem, p_send, p_recv, z_send, z_recv, f_send, f_recv, s_sem):
    me = lax.axis_index("fsdp")
    core = lax.rem(me, 2)
    partner = me + 1 - 2 * core
    experts, rows, columns = tg.shape
    width = columns // n
    trains, others, outs = (tg, tu), (og, ou), (rg, ru)

    def loads(x, o, x_sem, o_sem, e):
        slot = lax.rem(e, 2)
        copies = []
        for t in range(2):
            copies.append(pltpu.make_async_copy(trains[t].at[e], x.at[slot, t], x_sem.at[slot, t]))
            copies.append(pltpu.make_async_copy(others[t].at[e], o.at[slot, t], o_sem.at[slot, t]))
        return copies

    def remote(src, dst, send, recv, device):
        return pltpu.make_async_remote_copy(
            src_ref=src, dst_ref=dst, send_sem=send, recv_sem=recv, device_id={"fsdp": device},
            device_id_type=pl.DeviceIdType.MESH,
        )

    def wait_bytes(ref, sem):
        pltpu.make_async_copy(ref, ref, sem).wait()

    for copy in loads(mx, mo, mx_sem, mo_sem, 0):
        copy.start()
    for copy in loads(nx, no, nx_sem, no_sem, 0):
        copy.start()

    barrier = pltpu.get_barrier_semaphore()
    for k in range(1, n):
        pl.semaphore_signal(barrier, inc=1, device_id={"fsdp": lax.rem(me + k, n)}, device_id_type=pl.DeviceIdType.MESH)
    pl.semaphore_wait(barrier, n - 1)

    def measure(e):
        slot = lax.rem(e, 2)

        @pl.when(e + 1 < experts)
        def _():
            for copy in loads(mx, mo, mx_sem, mo_sem, e + 1):
                copy.start()

        for copy in loads(mx, mo, mx_sem, mo_sem, e):
            copy.wait()
        for t in range(2):
            for j in range(0, columns, LANES):
                latest = mx[slot, t, :, j : j + LANES] + mo[slot, t, :, j : j + LANES].astype(jnp.float32)
                own[e, t, :, j : j + LANES] = jnp.max(jnp.abs(latest), axis=0, keepdims=True)
        remote(own.at[e, 1 - core], pair.at[e], p_send.at[e], p_recv.at[e], partner).start()

    def chip_max(e):
        remote(own.at[e, 1 - core], pair.at[e], p_send.at[e], p_recv.at[e], partner).wait()
        both[e] = jnp.maximum(own[e, core], pair[e])
        for k in range(1, n // 2):
            remote(both.at[e], chips.at[e, k - 1], z_send.at[e], z_recv.at[e], lax.rem(me + 2 * k, n)).start()

    def all_max(e):
        wait_bytes(chips.at[e], z_send.at[e])
        wait_bytes(chips.at[e], z_recv.at[e])
        top = both[e]
        for k in range(1, n // 2):
            top = jnp.maximum(top, chips[e, k - 1])
        final[e, core] = top
        remote(final.at[e, core], final.at[e, core], f_send.at[e], f_recv.at[e], partner).start()

    def send(e):
        slot = lax.rem(e, 2)

        @pl.when(e + 1 < experts)
        def _():
            for copy in loads(nx, no, nx_sem, no_sem, e + 1):
                copy.start()

        for copy in loads(nx, no, nx_sem, no_sem, e):
            copy.wait()
        remote(final.at[e, core], final.at[e, core], f_send.at[e], f_recv.at[e], partner).wait()
        for t in range(2):
            for j in range(0, columns, LANES):
                latest = nx[slot, t, :, j : j + LANES] + no[slot, t, :, j : j + LANES].astype(jnp.float32)
                turned[j : j + LANES, :] = (latest / final[e, t, :, j : j + LANES]).T

            @pl.when(e >= 2)
            def _():
                wait_bytes(blocks.at[slot, t, pl.ds(0, n - 1)], send_sem.at[slot, t])
                wait_bytes(blocks.at[slot, t, 0], keep_sem.at[slot, t])

            for d in range(n):
                blocks[slot, t, d] = turned[d * width : (d + 1) * width, :].astype(jnp.bfloat16)
            place = outs[t].at[e, :, pl.ds(pl.multiple_of(me * rows, rows), rows)]
            for k in range(n):
                device = lax.rem(me + n // 2 + k, n)
                block = blocks.at[slot, t, device]
                if k == n // 2:
                    pltpu.make_async_copy(block, place, keep_sem.at[slot, t]).start()
                else:
                    remote(block, place, send_sem.at[slot, t], recv_sem.at[t, e], device).start()

    def step(i, carry):
        pl.when(i < experts)(lambda: measure(i))
        pl.when((i >= 1) & (i < experts + 1))(lambda: chip_max(i - 1))
        pl.when((i >= 2) & (i < experts + 2))(lambda: all_max(i - 2))
        pl.when(i >= DEPTH)(lambda: send(i - DEPTH))
        return carry

    lax.fori_loop(0, experts + DEPTH, step, 0)
    keep = pltpu.make_async_copy(final, scales, s_sem)
    keep.start()
    for slot in range(2):
        for t in range(2):
            wait_bytes(blocks.at[slot, t, pl.ds(0, n - 1)], send_sem.at[slot, t])
            wait_bytes(blocks.at[slot, t, 0], keep_sem.at[slot, t])

    def arrive(e, carry):
        for t in range(2):
            wait_bytes(outs[t].at[e, :, pl.ds(0, (n - 1) * rows)], recv_sem.at[t, e])
        return carry

    lax.fori_loop(0, experts, arrive, 0)
    keep.wait()


def per_device(n, train_gate, other_gate, train_up, other_up, router_weight, router_gain):
    experts, rows, columns = train_gate.shape
    width = columns // n
    f32, bf16, dma = jnp.float32, jnp.bfloat16, pltpu.SemaphoreType.DMA
    ready = jax.ShapeDtypeStruct((experts, width, rows * n), bf16)
    any_space = pl.BlockSpec(memory_space=pl.ANY)
    ready_gate, ready_up, scales = pl.pallas_call(
        functools.partial(regroup, n),
        out_shape=(ready, ready, jax.ShapeDtypeStruct((experts, 2, 1, columns), f32)),
        in_specs=[any_space] * 4,
        out_specs=(any_space,) * 3,
        scratch_shapes=[
            pltpu.VMEM((2, 2, rows, columns), f32),
            pltpu.VMEM((2, 2, rows, columns), bf16),
            pltpu.VMEM((2, 2, rows, columns), f32),
            pltpu.VMEM((2, 2, rows, columns), bf16),
            pltpu.VMEM((columns, rows), f32),
            pltpu.VMEM((2, 2, n, width, rows), bf16),
            pltpu.VMEM((experts, 2, 1, columns), f32),
            pltpu.VMEM((experts, 1, columns), f32),
            pltpu.VMEM((experts, 1, columns), f32),
            pltpu.VMEM((experts, n // 2 - 1, 1, columns), f32),
            pltpu.VMEM((experts, 2, 1, columns), f32),
            dma((2, 2)),
            dma((2, 2)),
            dma((2, 2)),
            dma((2, 2)),
            dma((2, 2)),
            dma((2, 2)),
            dma((2, experts)),
            dma((experts,)),
            dma((experts,)),
            dma((experts,)),
            dma((experts,)),
            dma((experts,)),
            dma((experts,)),
            dma,
        ],
        compiler_params=pltpu.CompilerParams(collective_id=0, has_side_effects=True, vmem_limit_bytes=48 * 2**20),
        name="regroup",
    )(train_gate, other_gate, train_up, other_up)
    ready_gate, ready_up = jnp.swapaxes(ready_gate, 1, 2), jnp.swapaxes(ready_up, 1, 2)
    mine = lax.dynamic_slice_in_dim(scales, lax.axis_index("fsdp") * width, width, axis=3)
    part_router = (router_weight * router_gain[:, None]).astype(jnp.bfloat16)
    row_router = lax.all_gather(part_router, "fsdp", axis=0, tiled=True)
    serve_router = lax.all_gather(row_router, "ep", axis=1, tiled=True)
    return (ready_gate, ready_up, mine[:, 0, 0], mine[:, 1, 0], serve_router)


def solution(mesh):
    in_specs = (
        P("ep", "fsdp", None),
        P("ep", "fsdp", None),
        P("ep", "fsdp", None),
        P("ep", "fsdp", None),
        P("fsdp", "ep"),
        P("fsdp"),
    )
    out_specs = (
        P("ep", None, "fsdp"),
        P("ep", None, "fsdp"),
        P("ep", "fsdp"),
        P("ep", "fsdp"),
        P(),
    )
    return jax.shard_map(
        functools.partial(per_device, mesh.shape["fsdp"]), mesh=mesh, in_specs=in_specs, out_specs=out_specs,
        check_vma=False,
    )
```

```python
import functools

import jax
import jax.numpy as jnp
from jax import lax
from jax.experimental import pallas as pl
from jax.experimental.pallas import tpu as pltpu
from jax.sharding import PartitionSpec as P

LANES = 128
DEPTH = 3


def regroup(n, teams, tg, og, tu, ou, part, rg, ru, scales, router, mx, mo, nx, no, turned, blocks, own, pair, both, chips, final,
            mx_sem, mo_sem, nx_sem, no_sem, send_sem, keep_sem, recv_sem, p_send, p_recv, z_send, z_recv, f_send, f_recv, s_sem,
            row, whole, a_send, a_recv, a_keep, b_send, b_recv, b_keep):
    me, team = lax.axis_index("fsdp"), lax.axis_index("ep")
    core = lax.rem(me, 2)
    partner = me + 1 - 2 * core
    experts, rows, columns = tg.shape
    width = columns // n
    trains, others, outs = (tg, tu), (og, ou), (rg, ru)

    def loads(x, o, x_sem, o_sem, e):
        slot = lax.rem(e, 2)
        copies = []
        for t in range(2):
            copies.append(pltpu.make_async_copy(trains[t].at[e], x.at[slot, t], x_sem.at[slot, t]))
            copies.append(pltpu.make_async_copy(others[t].at[e], o.at[slot, t], o_sem.at[slot, t]))
        return copies

    def remote(src, dst, send, recv, device):
        return pltpu.make_async_remote_copy(
            src_ref=src, dst_ref=dst, send_sem=send, recv_sem=recv, device_id={"fsdp": device},
            device_id_type=pl.DeviceIdType.MESH,
        )

    def wait_bytes(ref, sem):
        pltpu.make_async_copy(ref, ref, sem).wait()

    for copy in loads(mx, mo, mx_sem, mo_sem, 0):
        copy.start()
    for copy in loads(nx, no, nx_sem, no_sem, 0):
        copy.start()

    barrier = pltpu.get_barrier_semaphore()
    for k in range(1, n):
        pl.semaphore_signal(barrier, inc=1, device_id={"fsdp": lax.rem(me + k, n)}, device_id_type=pl.DeviceIdType.MESH)
    for k in range(1, teams):
        pl.semaphore_signal(barrier, inc=1, device_id={"ep": lax.rem(team + k, teams)}, device_id_type=pl.DeviceIdType.MESH)
    pl.semaphore_wait(barrier, n + teams - 2)

    def measure(e):
        slot = lax.rem(e, 2)

        @pl.when(e + 1 < experts)
        def _():
            for copy in loads(mx, mo, mx_sem, mo_sem, e + 1):
                copy.start()

        for copy in loads(mx, mo, mx_sem, mo_sem, e):
            copy.wait()
        for t in range(2):
            for j in range(0, columns, LANES):
                latest = mx[slot, t, :, j : j + LANES] + mo[slot, t, :, j : j + LANES].astype(jnp.float32)
                own[e, t, :, j : j + LANES] = jnp.max(jnp.abs(latest), axis=0, keepdims=True)
        remote(own.at[e, 1 - core], pair.at[e], p_send.at[e], p_recv.at[e], partner).start()

    def chip_max(e):
        remote(own.at[e, 1 - core], pair.at[e], p_send.at[e], p_recv.at[e], partner).wait()
        both[e] = jnp.maximum(own[e, core], pair[e])
        for k in range(1, n // 2):
            remote(both.at[e], chips.at[e, k - 1], z_send.at[e], z_recv.at[e], lax.rem(me + 2 * k, n)).start()

    def all_max(e):
        wait_bytes(chips.at[e], z_send.at[e])
        wait_bytes(chips.at[e], z_recv.at[e])
        top = both[e]
        for k in range(1, n // 2):
            top = jnp.maximum(top, chips[e, k - 1])
        final[e, core] = top
        remote(final.at[e, core], final.at[e, core], f_send.at[e], f_recv.at[e], partner).start()

    def send(e):
        slot = lax.rem(e, 2)

        @pl.when(e + 1 < experts)
        def _():
            for copy in loads(nx, no, nx_sem, no_sem, e + 1):
                copy.start()

        for copy in loads(nx, no, nx_sem, no_sem, e):
            copy.wait()
        remote(final.at[e, core], final.at[e, core], f_send.at[e], f_recv.at[e], partner).wait()
        for t in range(2):
            for j in range(0, columns, LANES):
                latest = nx[slot, t, :, j : j + LANES] + no[slot, t, :, j : j + LANES].astype(jnp.float32)
                turned[j : j + LANES, :] = (latest / final[e, t, :, j : j + LANES]).T

            @pl.when(e >= 2)
            def _():
                wait_bytes(blocks.at[slot, t, pl.ds(0, n - 1)], send_sem.at[slot, t])
                wait_bytes(blocks.at[slot, t, 0], keep_sem.at[slot, t])

            for d in range(n):
                blocks[slot, t, d] = turned[d * width : (d + 1) * width, :].astype(jnp.bfloat16)
            place = outs[t].at[e, :, pl.ds(pl.multiple_of(me * rows, rows), rows)]
            for k in range(n):
                device = lax.rem(me + n // 2 + k, n)
                block = blocks.at[slot, t, device]
                if k == n // 2:
                    pltpu.make_async_copy(block, place, keep_sem.at[slot, t]).start()
                else:
                    remote(block, place, send_sem.at[slot, t], recv_sem.at[t, e], device).start()

    def router_rows():
        pltpu.make_async_copy(part, row.at[me], a_keep).start()
        for k in range(1, n):
            remote(part, row.at[me], a_send, a_recv, lax.rem(me + k, n)).start()

    def router_columns():
        pltpu.make_async_copy(part, row.at[me], a_keep).wait()
        wait_bytes(row.at[pl.ds(0, n - 1)], a_send)
        wait_bytes(row.at[pl.ds(0, n - 1)], a_recv)
        pltpu.make_async_copy(row, whole.at[team], b_keep).start()
        for k in range(1, teams):
            pltpu.make_async_remote_copy(
                src_ref=row, dst_ref=whole.at[team], send_sem=b_send, recv_sem=b_recv,
                device_id={"ep": lax.rem(team + k, teams)}, device_id_type=pl.DeviceIdType.MESH,
            ).start()

    def step(i, carry):
        pl.when(i >= DEPTH)(lambda: send(i - DEPTH))
        pl.when(i < experts)(lambda: measure(i))
        pl.when((i >= 1) & (i < experts + 1))(lambda: chip_max(i - 1))
        pl.when((i >= 2) & (i < experts + 2))(lambda: all_max(i - 2))
        pl.when(i == DEPTH)(router_rows)
        pl.when(i == experts)(router_columns)
        return carry

    lax.fori_loop(0, experts + DEPTH, step, 0)
    keep = pltpu.make_async_copy(final, scales, s_sem)
    keep.start()
    pltpu.make_async_copy(row, whole.at[team], b_keep).wait()
    wait_bytes(whole.at[pl.ds(0, teams - 1)], b_send)
    wait_bytes(whole.at[pl.ds(0, teams - 1)], b_recv)
    keep_router = pltpu.make_async_copy(whole, router, a_keep)
    keep_router.start()
    for slot in range(2):
        for t in range(2):
            wait_bytes(blocks.at[slot, t, pl.ds(0, n - 1)], send_sem.at[slot, t])
            wait_bytes(blocks.at[slot, t, 0], keep_sem.at[slot, t])

    def arrive(e, carry):
        for t in range(2):
            wait_bytes(outs[t].at[e, :, pl.ds(0, (n - 1) * rows)], recv_sem.at[t, e])
        return carry

    lax.fori_loop(0, experts, arrive, 0)
    keep.wait()
    keep_router.wait()


def per_device(n, teams, train_gate, other_gate, train_up, other_up, router_weight, router_gain):
    experts, rows, columns = train_gate.shape
    width = columns // n
    f32, bf16, dma = jnp.float32, jnp.bfloat16, pltpu.SemaphoreType.DMA
    ready = jax.ShapeDtypeStruct((experts, width, rows * n), bf16)
    any_space = pl.BlockSpec(memory_space=pl.ANY)
    part_router = (router_weight * router_gain[:, None]).astype(bf16).T
    ready_gate, ready_up, scales, router = pl.pallas_call(
        functools.partial(regroup, n, teams),
        out_shape=(ready, ready, jax.ShapeDtypeStruct((experts, 2, 1, columns), f32),
                   jax.ShapeDtypeStruct((teams, n) + part_router.shape, bf16)),
        in_specs=[any_space] * 4 + [pl.BlockSpec(memory_space=pltpu.VMEM)],
        out_specs=(any_space,) * 4,
        scratch_shapes=[
            pltpu.VMEM((2, 2, rows, columns), f32),
            pltpu.VMEM((2, 2, rows, columns), bf16),
            pltpu.VMEM((2, 2, rows, columns), f32),
            pltpu.VMEM((2, 2, rows, columns), bf16),
            pltpu.VMEM((columns, rows), f32),
            pltpu.VMEM((2, 2, n, width, rows), bf16),
            pltpu.VMEM((experts, 2, 1, columns), f32),
            pltpu.VMEM((experts, 1, columns), f32),
            pltpu.VMEM((experts, 1, columns), f32),
            pltpu.VMEM((experts, n // 2 - 1, 1, columns), f32),
            pltpu.VMEM((experts, 2, 1, columns), f32),
            dma((2, 2)),
            dma((2, 2)),
            dma((2, 2)),
            dma((2, 2)),
            dma((2, 2)),
            dma((2, 2)),
            dma((2, experts)),
            dma((experts,)),
            dma((experts,)),
            dma((experts,)),
            dma((experts,)),
            dma((experts,)),
            dma((experts,)),
            dma,
            pltpu.VMEM((n,) + part_router.shape, bf16),
            pltpu.VMEM((teams, n) + part_router.shape, bf16),
            dma,
            dma,
            dma,
            dma,
            dma,
            dma,
        ],
        compiler_params=pltpu.CompilerParams(collective_id=0, has_side_effects=True, vmem_limit_bytes=48 * 2**20),
        name="regroup",
    )(train_gate, other_gate, train_up, other_up, part_router)
    ready_gate, ready_up = jnp.swapaxes(ready_gate, 1, 2), jnp.swapaxes(ready_up, 1, 2)
    mine = lax.dynamic_slice_in_dim(scales, lax.axis_index("fsdp") * width, width, axis=3)
    serve_router = router.transpose(1, 3, 0, 2).reshape(n * router.shape[3], -1)
    return (ready_gate, ready_up, mine[:, 0, 0], mine[:, 1, 0], serve_router)


def solution(mesh):
    in_specs = (
        P("ep", "fsdp", None),
        P("ep", "fsdp", None),
        P("ep", "fsdp", None),
        P("ep", "fsdp", None),
        P("fsdp", "ep"),
        P("fsdp"),
    )
    out_specs = (
        P("ep", None, "fsdp"),
        P("ep", None, "fsdp"),
        P("ep", "fsdp"),
        P("ep", "fsdp"),
        P(),
    )
    return jax.shard_map(
        functools.partial(per_device, mesh.shape["fsdp"], mesh.shape["ep"]), mesh=mesh, in_specs=in_specs, out_specs=out_specs,
        check_vma=False,
    )
```
